8 devices in a mesh: dp: 4 (over z, y, x), cp: 2 (over core).
Axes of the slice: x: 2, y: 2, z: 1, core: 2. Of those that a mesh axis runs over, the one named last changes fastest.
Arguments:
- x_in: bfloat16 [32, 512, 2048], P('dp', 'cp')
- d_out: bfloat16 [32, 512, 2048], P('dp', 'cp')
- w_q: bfloat16 [2048, 32, 64], replicated
- w_k: bfloat16 [2048, 4, 64], replicated
- w_v: bfloat16 [2048, 4, 64], replicated
- w_o: bfloat16 [32, 64, 2048], replicated
- w_up: bfloat16 [2048, 5632], replicated
- w_down: bfloat16 [5632, 2048], replicated
Outputs:
- output 1: bfloat16 [32, 512, 2048], P('dp', 'cp')
- output 2: float32 [2048, 32, 64], replicated
- output 3: float32 [2048, 4, 64], replicated
- output 4: float32 [2048, 4, 64], replicated
- output 5: float32 [32, 64, 2048], replicated
- output 6: float32 [2048, 5632], replicated
- output 7: float32 [5632, 2048], replicated
All inputs are finite; a program needn't handle non-finite values.
Results may differ from the reference program's by a relative error of at most 0.02.
Values are sent between devices in bfloat16 or wider.
A program may use at most 1 GiB of HBM per device.

```python
import jax
import jax.numpy as jnp
from jax import lax

MODEL_WIDTH = 2048
NUM_HEADS = 32
KV_HEADS = 4
HEAD_DIM = 64
FFN_WIDTH = 5632
BATCH_SIZE = 32
SEQ_LEN = 512
QUERY_BLOCK = 256
GRAD_DIVISOR = 8

GROUP_SIZE = NUM_HEADS // KV_HEADS
SCORE_SCALE = HEAD_DIM ** -0.5


def setup_inputs(seed: int = 0) -> dict:
    rng_keys = jax.random.split(jax.random.key(seed), 8)
    act_shape = (BATCH_SIZE, SEQ_LEN, MODEL_WIDTH)

    def draw_weight(one_key, shape, fan_in, weight_gain):
        values = jax.random.normal(one_key, shape, jnp.float32) * (weight_gain * fan_in ** -0.5)
        return values.astype(jnp.bfloat16)

    return {
        'x_in': jax.random.normal(rng_keys[0], act_shape, jnp.float32).astype(jnp.bfloat16),
        'd_out': jax.random.normal(rng_keys[1], act_shape, jnp.float32).astype(jnp.bfloat16),
        'w_q': draw_weight(rng_keys[2], (MODEL_WIDTH, NUM_HEADS, HEAD_DIM), MODEL_WIDTH, 2.5),
        'w_k': draw_weight(rng_keys[3], (MODEL_WIDTH, KV_HEADS, HEAD_DIM), MODEL_WIDTH, 1.0),
        'w_v': draw_weight(rng_keys[4], (MODEL_WIDTH, KV_HEADS, HEAD_DIM), MODEL_WIDTH, 1.0),
        'w_o': draw_weight(rng_keys[5], (NUM_HEADS, HEAD_DIM, MODEL_WIDTH), NUM_HEADS * HEAD_DIM, 1.5),
        'w_up': draw_weight(rng_keys[6], (MODEL_WIDTH, FFN_WIDTH), MODEL_WIDTH, 1.0),
        'w_down': draw_weight(rng_keys[7], (FFN_WIDTH, MODEL_WIDTH), FFN_WIDTH, 1.0),
    }


def block_attention(q_block, k_seq, v_seq):
    scores = jnp.einsum('qkgd,pkd->kgqp', q_block, k_seq) * SCORE_SCALE
    prob_rounded = jax.nn.softmax(scores, axis=-1).astype(jnp.bfloat16).astype(jnp.float32)
    return jnp.einsum('kgqp,pkd->qkgd', prob_rounded, v_seq)


checked_attention = jax.checkpoint(block_attention)


def attend_sequence(operands):
    q_seq, k_seq, v_seq = operands
    q_blocks = q_seq.reshape(SEQ_LEN // QUERY_BLOCK, QUERY_BLOCK, KV_HEADS, GROUP_SIZE, HEAD_DIM)
    out_blocks = lax.map(lambda q_block: checked_attention(q_block, k_seq, v_seq), q_blocks)
    return out_blocks.reshape(SEQ_LEN, KV_HEADS, GROUP_SIZE, HEAD_DIM)


def layer_forward(x_in, w_q, w_k, w_v, w_o, w_up, w_down):
    row_count = BATCH_SIZE * SEQ_LEN
    x_rows = x_in.reshape(row_count, MODEL_WIDTH).astype(jnp.float32)

    def project(weight, head_count):
        product = jnp.dot(x_rows, weight.reshape(MODEL_WIDTH, head_count * HEAD_DIM), preferred_element_type=jnp.float32)
        return product.astype(jnp.bfloat16).astype(jnp.float32)

    q_all = project(w_q, NUM_HEADS).reshape(BATCH_SIZE, SEQ_LEN, KV_HEADS, GROUP_SIZE, HEAD_DIM)
    k_all = project(w_k, KV_HEADS).reshape(BATCH_SIZE, SEQ_LEN, KV_HEADS, HEAD_DIM)
    v_all = project(w_v, KV_HEADS).reshape(BATCH_SIZE, SEQ_LEN, KV_HEADS, HEAD_DIM)
    attn_out = lax.map(attend_sequence, (q_all, k_all, v_all))
    attn_rows = attn_out.astype(jnp.bfloat16).astype(jnp.float32).reshape(row_count, NUM_HEADS * HEAD_DIM)
    out_proj = jnp.dot(attn_rows, w_o.reshape(NUM_HEADS * HEAD_DIM, MODEL_WIDTH), preferred_element_type=jnp.float32)
    hidden = (x_rows + out_proj).astype(jnp.bfloat16).astype(jnp.float32)
    up_proj = jnp.dot(hidden, w_up, preferred_element_type=jnp.float32)
    gated = jax.nn.gelu(up_proj, approximate=True).astype(jnp.bfloat16).astype(jnp.float32)
    out_rows = hidden + jnp.dot(gated, w_down, preferred_element_type=jnp.float32)
    return out_rows.astype(jnp.bfloat16).reshape(BATCH_SIZE, SEQ_LEN, MODEL_WIDTH)


def reference(x_in, d_out, w_q, w_k, w_v, w_o, w_up, w_down):
    layer_vjp = jax.vjp(layer_forward, x_in, w_q.astype(jnp.float32), w_k.astype(jnp.float32), w_v.astype(jnp.float32), w_o.astype(jnp.float32), w_up.astype(jnp.float32), w_down.astype(jnp.float32))[1]
    cotangents = layer_vjp(d_out)
    return (cotangents[0], cotangents[1] / GRAD_DIVISOR, cotangents[2] / GRAD_DIVISOR, cotangents[3] / GRAD_DIVISOR, cotangents[4] / GRAD_DIVISOR, cotangents[5] / GRAD_DIVISOR, cotangents[6] / GRAD_DIVISOR)
```

```python
import functools
import jax
import jax.numpy as jnp
from jax import lax
from jax.experimental import pallas as pl
from jax.sharding import PartitionSpec as P


F32, BF16 = jnp.float32, jnp.bfloat16
LOG2E = 1.4426950408889634


def dot(a, b, ca, cb):
    return lax.dot_general(a, b, (((ca,), (cb,)), ((), ())), preferred_element_type=F32)


def join_keys(own_ref, other_ref, lo, width):
    return jnp.concatenate([own_ref[:, lo:lo + width], other_ref[:, lo:lo + width]], axis=0)


def attn_fwd_kernel(group, head_dim, q_ref, k_own, k_oth, v_own, v_oth, out_ref, lse_ref):
    coef = head_dim ** -0.5 * LOG2E
    for kv in range(2):
        keys = join_keys(k_own, k_oth, kv * head_dim, head_dim)
        vals = join_keys(v_own, v_oth, kv * head_dim, head_dim)
        outs = []
        for g in range(group):
            head = kv * group + g
            q = q_ref[:, head * head_dim:(head + 1) * head_dim]
            scores = dot(keys, q, 1, 1)
            top = jnp.max(scores, axis=0, keepdims=True)
            probs = jnp.exp2((scores - top) * coef)
            total = jnp.sum(probs, axis=0, keepdims=True)
            out_t = dot(vals, probs.astype(BF16), 0, 0)
            outs.append(out_t * (1.0 / total))
            lse_ref[0, head:head + 1, :] = top * coef + jnp.log(total) * LOG2E
        width = group * head_dim
        out_ref[:, kv * width:(kv + 1) * width] = jnp.concatenate(outs, axis=0).T.astype(BF16)


def attn_bwd_kernel(group, head_dim, q_ref, k_own, k_oth, v_own, v_oth, do_ref, lse_ref, dq_ref, dk_own, dk_oth, dv_own, dv_oth):
    scale = head_dim ** -0.5
    coef = scale * LOG2E
    seq = q_ref.shape[0]
    for kv in range(2):
        keys = join_keys(k_own, k_oth, kv * head_dim, head_dim)
        vals = join_keys(v_own, v_oth, kv * head_dim, head_dim)
        dk = dv = None
        dqs = []
        for g in range(group):
            head = kv * group + g
            cols = slice(head * head_dim, (head + 1) * head_dim)
            q = q_ref[:, cols]
            d_out = do_ref[:, cols]
            probs = jnp.exp2(dot(keys, q, 1, 1) * coef - lse_ref[0, head:head + 1, :])
            d_probs = dot(vals, d_out, 1, 1)
            weighted = probs * d_probs
            delta = jnp.sum(weighted, axis=0, keepdims=True)
            d_scores = (weighted - probs * delta).astype(BF16)
            dv_part = dot(probs.astype(BF16), d_out, 1, 0)
            dk_part = dot(d_scores, q, 1, 0)
            dv = dv_part if dv is None else dv + dv_part
            dk = dk_part if dk is None else dk + dk_part
            dqs.append(dot(keys, d_scores, 0, 0))
        width = group * head_dim
        dq_ref[:, kv * width:(kv + 1) * width] = (jnp.concatenate(dqs, axis=0) * scale).T.astype(BF16)
        lanes = slice(kv * head_dim, (kv + 1) * head_dim)
        dk_own[:, lanes] = dk[:seq] * scale
        dk_oth[:, lanes] = dk[seq:] * scale
        dv_own[:, lanes] = dv[:seq]
        dv_oth[:, lanes] = dv[seq:]


def attention_specs(seq, group, head_dim, kv_heads):
    pairs = kv_heads // 2
    q_spec = pl.BlockSpec((seq, 2 * group * head_dim), lambda b, p: (b, p))
    k_spec = pl.BlockSpec((seq, 2 * head_dim), lambda b, p: (b, p))
    v_spec = pl.BlockSpec((seq, 2 * head_dim), lambda b, p: (b, pairs + p))
    lse_spec = pl.BlockSpec((1, 2 * group, seq), lambda b, p: (b, p, 0))
    return q_spec, k_spec, v_spec, lse_spec


def attention_forward(q, kv_own, kv_oth, batch, seq, heads, kv_heads, head_dim):
    group = heads // kv_heads
    q_spec, k_spec, v_spec, lse_spec = attention_specs(seq, group, head_dim, kv_heads)
    return pl.pallas_call(
        functools.partial(attn_fwd_kernel, group, head_dim),
        grid=(batch, kv_heads // 2),
        in_specs=[q_spec, k_spec, k_spec, v_spec, v_spec],
        out_specs=[q_spec, lse_spec],
        out_shape=[jax.ShapeDtypeStruct(q.shape, BF16), jax.ShapeDtypeStruct((batch, heads, seq), F32)],
        cost_estimate=pl.CostEstimate(flops=40_000_000_000, bytes_accessed=25_000_000, transcendentals=33_000_000),
        name="attn_fwd",
    )(q, kv_own, kv_oth, kv_own, kv_oth)


def attention_backward(q, kv_own, kv_oth, d_attn, lse, batch, seq, heads, kv_heads, head_dim):
    group = heads // kv_heads
    q_spec, k_spec, v_spec, lse_spec = attention_specs(seq, group, head_dim, kv_heads)
    kv_grad = jax.ShapeDtypeStruct((batch * seq, kv_heads * head_dim), F32)
    return pl.pallas_call(
        functools.partial(attn_bwd_kernel, group, head_dim),
        grid=(batch, kv_heads // 2),
        in_specs=[q_spec, k_spec, k_spec, v_spec, v_spec, q_spec, lse_spec],
        out_specs=[q_spec, k_spec, k_spec, k_spec, k_spec],
        out_shape=[jax.ShapeDtypeStruct(q.shape, BF16), kv_grad, kv_grad, kv_grad, kv_grad],
        cost_estimate=pl.CostEstimate(flops=100_000_000_000, bytes_accessed=40_000_000, transcendentals=33_000_000),
        name="attn_bwd",
    )(q, kv_own, kv_oth, kv_own, kv_oth, d_attn, lse)


def solution(mesh):
    dp_size, cp_size = mesh.shape['dp'], mesh.shape['cp']
    assert dp_size == 4 and cp_size == 2
    grad_scale = 1.0 / (dp_size * cp_size)
    first_bit = [1, 2]
    swap_cores = [(c, 1 - c) for c in range(2)]
    both = ('dp', 'cp')

    def pairs(bits):
        return [(2 * d + c, 2 * (d ^ bits[c]) + c) for d in range(4) for c in range(2)]

    first_perm, second_perm = pairs(first_bit), pairs(first_bit[::-1])

    def to_other_core(arrays):
        return lax.ppermute(arrays, 'cp', swap_cores)

    def device_backward(x_in, d_out, w_q, w_k, w_v, w_o, w_up, w_down):
        batch, seq, width = x_in.shape
        heads, head_dim = w_q.shape[1], w_q.shape[2]
        kv_heads = w_k.shape[1]
        rows = batch * seq
        dims = (batch, seq, heads, kv_heads, head_dim)
        x = x_in.reshape(rows, width)
        dout = d_out.reshape(rows, width)
        wq_t = w_q.transpose(1, 2, 0).reshape(heads * head_dim, width)
        wk_t = w_k.transpose(1, 2, 0).reshape(kv_heads * head_dim, width)
        wv_t = w_v.transpose(1, 2, 0).reshape(kv_heads * head_dim, width)
        wkv_t = jnp.concatenate([wk_t, wv_t], axis=0)
        wo = w_o.reshape(heads * head_dim, width)

        chip, core = lax.axis_index('dp'), lax.axis_index('cp')

        def block_order(c):
            bit = 1 + c
            return [(chip ^ 3) * 2 + c, (chip ^ bit) * 2 + c, (chip ^ (3 - bit)) * 2 + c, chip * 2 + c]

        own_order, other_order = block_order(core), block_order(1 - core)

        def take(array, order, axis):
            size = array.shape[axis] // (dp_size * cp_size)
            return jnp.concatenate([lax.dynamic_slice_in_dim(array, i * size, size, axis) for i in order], axis=axis)

        def reduce_block(left, axis, left_oth, right, right_oth, right_axis):
            half = left_oth.shape[axis] // 2

            def own_product(part):
                own = take(left, own_order[2 * part:2 * part + 2], axis)
                return dot(own, right, 1 - axis, right_axis)

            def product(part, own):
                oth = lax.slice_in_dim(left_oth, part * half, (part + 1) * half, axis=axis)
                return own + dot(oth, right_oth, 1 - axis, right_axis)

            own0, own1 = own_product(0), own_product(1)
            arrived = lax.ppermute(product(0, own0), both, first_perm)
            kept = product(1, own1)
            size = kept.shape[0] // 2
            arrived2 = lax.ppermute(kept[:size] + arrived[:size], both, second_perm)
            return kept[size:] + arrived[size:] + arrived2

        def gather(block):
            return lax.all_gather(block, both, axis=0, tiled=True) * grad_scale

        kv = dot(x, wkv_t, 1, 1).astype(BF16)
        kv_oth = to_other_core(kv)
        x_oth = to_other_core(x)
        dout_oth = to_other_core(dout)
        q = dot(x, wq_t, 1, 1).astype(BF16)
        attn, lse = attention_forward(q, kv, kv_oth, *dims)
        attn_oth = to_other_core(take(attn, other_order, 1))
        hidden = (x.astype(F32) + dot(attn, wo, 1, 0)).astype(BF16)
        hid_oth = to_other_core(take(hidden, other_order, 1))
        up_t = dot(w_up, hidden, 0, 1)
        gated, gelu_vjp = jax.vjp(functools.partial(jax.nn.gelu, approximate=True), up_t)
        gated = gated.astype(BF16)
        gated_oth = to_other_core(take(gated, other_order, 0))

        dn_block = reduce_block(gated, 0, gated_oth, dout, dout_oth, 0)
        d_gated = dot(w_down, dout, 1, 1).astype(BF16)
        d_up = gelu_vjp(d_gated.astype(F32))[0].astype(BF16)
        dup_oth = to_other_core(d_up)
        up_block = reduce_block(hidden, 1, hid_oth, d_up, dup_oth, 1)
        d_hid = (dout.astype(F32) + dot(d_up, w_up, 0, 1)).astype(BF16)
        dhid_oth = to_other_core(d_hid)
        o_block = reduce_block(attn, 1, attn_oth, d_hid, dhid_oth, 0)
        d_attn = dot(d_hid, wo, 1, 1).astype(BF16)
        d_attn, dn_block = lax.optimization_barrier((d_attn, dn_block))
        dq, dk, dk_send, dv, dv_send = attention_backward(q, kv, kv_oth, d_attn, lse, *dims)
        dq_oth = to_other_core(take(dq, other_order, 1))
        dk_arr = to_other_core(dk_send)
        dv_arr = to_other_core(dv_send)
        d_kv = jnp.concatenate([(dk + dk_arr).astype(BF16), (dv + dv_arr).astype(BF16)], axis=1)
        q_block = reduce_block(dq, 1, dq_oth, x, x_oth, 0)
        dw_kv = lax.psum(dot(d_kv, x, 0, 0), both) * grad_scale
        d_x = d_hid.astype(F32) + dot(dq, wq_t, 1, 0) + dot(d_kv, wkv_t, 1, 0)
        d_x = d_x.astype(BF16).reshape(x_in.shape)

        dw_down, dw_up = gather(dn_block), gather(up_block)
        dw_o, dw_q = gather(o_block), gather(q_block)

        def weight_shape(grad_t, weight):
            return grad_t.reshape(weight.shape[1], weight.shape[2], width).transpose(2, 0, 1)

        kv_rows = kv_heads * head_dim
        return (d_x, weight_shape(dw_q, w_q), weight_shape(dw_kv[:kv_rows], w_k), weight_shape(dw_kv[kv_rows:], w_v), dw_o.reshape(w_o.shape), dw_up, dw_down)

    act_spec = P('dp', 'cp', None)
    return jax.shard_map(device_backward, mesh=mesh, in_specs=(act_spec, act_spec, P(), P(), P(), P(), P(), P()), out_specs=(act_spec, P(), P(), P(), P(), P(), P()), check_vma=False)
```

```python
import functools
import jax
import jax.numpy as jnp
from jax import lax
from jax.experimental import pallas as pl
from jax.sharding import PartitionSpec as P


F32, BF16 = jnp.float32, jnp.bfloat16
LOG2E = 1.4426950408889634


def dot(a, b, ca, cb):
    return lax.dot_general(a, b, (((ca,), (cb,)), ((), ())), preferred_element_type=F32)


def join_keys(own_ref, other_ref, lo, width):
    return jnp.concatenate([own_ref[:, lo:lo + width], other_ref[:, lo:lo + width]], axis=0)


def attn_fwd_kernel(group, head_dim, q_ref, k_own, k_oth, v_own, v_oth, out_ref, lse_ref):
    coef = head_dim ** -0.5 * LOG2E
    for kv in range(2):
        keys = join_keys(k_own, k_oth, kv * head_dim, head_dim)
        vals = join_keys(v_own, v_oth, kv * head_dim, head_dim)
        outs = []
        for g in range(group):
            head = kv * group + g
            q = q_ref[:, head * head_dim:(head + 1) * head_dim]
            scores = dot(keys, q, 1, 1)
            top = jnp.max(scores, axis=0, keepdims=True)
            probs = jnp.exp2((scores - top) * coef)
            total = jnp.sum(probs, axis=0, keepdims=True)
            out_t = dot(vals, probs.astype(BF16), 0, 0)
            outs.append(out_t * (1.0 / total))
            lse_ref[0, head:head + 1, :] = top * coef + jnp.log(total) * LOG2E
        width = group * head_dim
        out_ref[:, kv * width:(kv + 1) * width] = jnp.concatenate(outs, axis=0).T.astype(BF16)


def attn_bwd_kernel(group, head_dim, q_ref, k_own, k_oth, v_own, v_oth, do_ref, lse_ref, dq_ref, dk_own, dk_oth, dv_own, dv_oth):
    scale = head_dim ** -0.5
    coef = scale * LOG2E
    seq = q_ref.shape[0]
    for kv in range(2):
        keys = join_keys(k_own, k_oth, kv * head_dim, head_dim)
        vals = join_keys(v_own, v_oth, kv * head_dim, head_dim)
        dk = dv = None
        dqs = []
        for g in range(group):
            head = kv * group + g
            cols = slice(head * head_dim, (head + 1) * head_dim)
            q = q_ref[:, cols]
            d_out = do_ref[:, cols]
            probs = jnp.exp2(dot(keys, q, 1, 1) * coef - lse_ref[0, head:head + 1, :])
            d_probs = dot(vals, d_out, 1, 1)
            weighted = probs * d_probs
            delta = jnp.sum(weighted, axis=0, keepdims=True)
            d_scores = (weighted - probs * delta).astype(BF16)
            dv_part = dot(probs.astype(BF16), d_out, 1, 0)
            dk_part = dot(d_scores, q, 1, 0)
            dv = dv_part if dv is None else dv + dv_part
            dk = dk_part if dk is None else dk + dk_part
            dqs.append(dot(keys, d_scores, 0, 0))
        width = group * head_dim
        dq_ref[:, kv * width:(kv + 1) * width] = (jnp.concatenate(dqs, axis=0) * scale).T.astype(BF16)
        lanes = slice(kv * head_dim, (kv + 1) * head_dim)
        dk_own[:, lanes] = dk[:seq] * scale
        dk_oth[:, lanes] = dk[seq:] * scale
        dv_own[:, lanes] = dv[:seq]
        dv_oth[:, lanes] = dv[seq:]


def attention_specs(seq, group, head_dim, kv_heads):
    pairs = kv_heads // 2
    q_spec = pl.BlockSpec((seq, 2 * group * head_dim), lambda b, p: (b, p))
    k_spec = pl.BlockSpec((seq, 2 * head_dim), lambda b, p: (b, p))
    v_spec = pl.BlockSpec((seq, 2 * head_dim), lambda b, p: (b, pairs + p))
    lse_spec = pl.BlockSpec((1, 2 * group, seq), lambda b, p: (b, p, 0))
    return q_spec, k_spec, v_spec, lse_spec


def attention_forward(q, kv_own, kv_oth, batch, seq, heads, kv_heads, head_dim):
    group = heads // kv_heads
    q_spec, k_spec, v_spec, lse_spec = attention_specs(seq, group, head_dim, kv_heads)
    return pl.pallas_call(
        functools.partial(attn_fwd_kernel, group, head_dim),
        grid=(batch, kv_heads // 2),
        in_specs=[q_spec, k_spec, k_spec, v_spec, v_spec],
        out_specs=[q_spec, lse_spec],
        out_shape=[jax.ShapeDtypeStruct(q.shape, BF16), jax.ShapeDtypeStruct((batch, heads, seq), F32)],
        cost_estimate=pl.CostEstimate(flops=40_000_000_000, bytes_accessed=25_000_000, transcendentals=33_000_000),
        name="attn_fwd",
    )(q, kv_own, kv_oth, kv_own, kv_oth)


def attention_backward(q, kv_own, kv_oth, d_attn, lse, batch, seq, heads, kv_heads, head_dim):
    group = heads // kv_heads
    q_spec, k_spec, v_spec, lse_spec = attention_specs(seq, group, head_dim, kv_heads)
    kv_grad = jax.ShapeDtypeStruct((batch * seq, kv_heads * head_dim), F32)
    return pl.pallas_call(
        functools.partial(attn_bwd_kernel, group, head_dim),
        grid=(batch, kv_heads // 2),
        in_specs=[q_spec, k_spec, k_spec, v_spec, v_spec, q_spec, lse_spec],
        out_specs=[q_spec, k_spec, k_spec, k_spec, k_spec],
        out_shape=[jax.ShapeDtypeStruct(q.shape, BF16), kv_grad, kv_grad, kv_grad, kv_grad],
        cost_estimate=pl.CostEstimate(flops=100_000_000_000, bytes_accessed=40_000_000, transcendentals=33_000_000),
        name="attn_bwd",
    )(q, kv_own, kv_oth, kv_own, kv_oth, d_attn, lse)


def solution(mesh):
    dp_size, cp_size = mesh.shape['dp'], mesh.shape['cp']
    assert dp_size == 4 and cp_size == 2
    grad_scale = 1.0 / (dp_size * cp_size)
    first_bit = [1, 2]
    swap_cores = [(c, 1 - c) for c in range(2)]
    both = ('dp', 'cp')

    def pairs(bits):
        return [(2 * d + c, 2 * (d ^ bits[c]) + c) for d in range(4) for c in range(2)]

    first_perm, second_perm = pairs(first_bit), pairs(first_bit[::-1])

    def to_other_core(arrays):
        return lax.ppermute(arrays, 'cp', swap_cores)

    def device_backward(x_in, d_out, w_q, w_k, w_v, w_o, w_up, w_down):
        batch, seq, width = x_in.shape
        heads, head_dim = w_q.shape[1], w_q.shape[2]
        kv_heads = w_k.shape[1]
        rows = batch * seq
        dims = (batch, seq, heads, kv_heads, head_dim)
        x = x_in.reshape(rows, width)
        dout = d_out.reshape(rows, width)
        wq_t = w_q.transpose(1, 2, 0).reshape(heads * head_dim, width)
        wk_t = w_k.transpose(1, 2, 0).reshape(kv_heads * head_dim, width)
        wv_t = w_v.transpose(1, 2, 0).reshape(kv_heads * head_dim, width)
        wkv_t = jnp.concatenate([wk_t, wv_t], axis=0)
        wo = w_o.reshape(heads * head_dim, width)

        chip, core = lax.axis_index('dp'), lax.axis_index('cp')

        def block_order(c):
            bit = 1 + c
            return [(chip ^ 3) * 2 + c, (chip ^ bit) * 2 + c, (chip ^ (3 - bit)) * 2 + c, chip * 2 + c]

        own_order, other_order = block_order(core), block_order(1 - core)

        def take(array, order, axis):
            size = array.shape[axis] // (dp_size * cp_size)
            return jnp.concatenate([lax.dynamic_slice_in_dim(array, i * size, size, axis) for i in order], axis=axis)

        def block_of(array, i, axis):
            size = array.shape[axis] // (dp_size * cp_size)
            return lax.dynamic_slice_in_dim(array, i * size, size, axis)

        def own_products(left, right, right_axis):
            parts = [take(left, own_order[p:p + 2], 1) for p in (0, 2)]
            return [lax.optimization_barrier(dot(part, right, 0, right_axis)) for part in parts]

        def add_product(part, own, left_oth, right_oth, right_axis):
            half = left_oth.shape[1] // 2
            oth = left_oth[:, part * half:(part + 1) * half]
            return own + dot(oth, right_oth, 0, right_axis)

        def first_exchange(sent, kept):
            arrived = lax.ppermute(sent, both, first_perm)
            size = kept.shape[0] // 2
            return kept[:size] + arrived[:size], (kept[size:], arrived[size:])

        def second_exchange(middle, rest):
            return rest[0] + rest[1] + lax.ppermute(middle, both, second_perm)

        def gather(block):
            return lax.all_gather(block, both, axis=0, tiled=True)

        kv = dot(x, wkv_t, 1, 1).astype(BF16)
        kv_oth = to_other_core(kv)
        dout_oth = to_other_core(dout)
        q = dot(x, wq_t, 1, 1).astype(BF16)
        attn, lse = attention_forward(q, kv, kv_oth, *dims)
        hidden = (x.astype(F32) + dot(attn, wo, 1, 0)).astype(BF16)
        up_t = dot(w_up, hidden, 0, 1)
        gated, gelu_vjp = jax.vjp(functools.partial(jax.nn.gelu, approximate=True), up_t)
        gated = gated.astype(BF16)
        gated_oths = [to_other_core(block_of(gated, i, 0)) for i in other_order]

        def dn_product(i, own):
            return own + dot(gated_oths[i], dout_oth, 1, 0)

        dn_own = [lax.optimization_barrier(dot(block_of(gated, i, 0), dout, 1, 0)) for i in own_order]
        dn_sent = dn_product(0, dn_own[0])
        arrived_a = lax.ppermute(dn_sent, both, first_perm)
        arrived_b = lax.ppermute(dn_product(1, dn_own[1]), both, first_perm)
        dn_middle = dn_product(2, dn_own[2]) + arrived_a
        dn_block = second_exchange(dn_middle, (dn_product(3, dn_own[3]), arrived_b))

        d_gated = dot(w_down, dout, 1, 1).astype(BF16)
        d_up = gelu_vjp(d_gated.astype(F32))[0].astype(BF16)
        dup_oth = to_other_core(d_up)
        d_up, dn_block, hid_late, attn_late = lax.optimization_barrier((d_up, dn_block, hidden, attn))
        hid_oth = to_other_core(take(hid_late, other_order, 1))
        attn_oth = to_other_core(take(attn_late, other_order, 1))
        up_own = own_products(hid_late, d_up, 1)
        up_sent = add_product(0, up_own[0], hid_oth, dup_oth, 1)
        up_kept = add_product(1, up_own[1], hid_oth, dup_oth, 1)
        up_middle, up_rest = first_exchange(up_sent, up_kept)

        d_hid = (dout.astype(F32) + dot(d_up, w_up, 0, 1)).astype(BF16)
        dhid_oth = to_other_core(d_hid)
        d_attn = dot(d_hid, wo, 1, 1).astype(BF16)
        o_own = own_products(attn_late, d_hid, 0)
        o_sent = add_product(0, o_own[0], attn_oth, dhid_oth, 0)
        x_late, d_attn, o_sent, up_middle = lax.optimization_barrier((x, d_attn, o_sent, up_middle))
        o_kept = add_product(1, o_own[1], attn_oth, dhid_oth, 0)
        o_middle, o_rest = first_exchange(o_sent, o_kept)
        up_block = second_exchange(up_middle, up_rest)
        x_oth = to_other_core(x_late)

        dq, dk, dk_send, dv, dv_send = attention_backward(q, kv, kv_oth, d_attn, lse, *dims)
        dq, o_middle, up_block = lax.optimization_barrier((dq, o_middle, up_block))
        o_block = second_exchange(o_middle, o_rest)
        dq_oth = to_other_core(take(dq, other_order, 1))
        dk_arr = to_other_core(dk_send)
        dv_arr = to_other_core(dv_send)
        d_kv = jnp.concatenate([(dk + dk_arr).astype(BF16), (dv + dv_arr).astype(BF16)], axis=1)
        q_own = own_products(dq, x_late, 0)
        q_sent = add_product(0, q_own[0], dq_oth, x_oth, 0)
        q_kept = add_product(1, q_own[1], dq_oth, x_oth, 0)
        q_block = second_exchange(*first_exchange(q_sent, q_kept))
        dw_kv = dot(d_kv, x_late, 0, 0)
        dw_kv = take(dw_kv, own_order, 0) + to_other_core(take(dw_kv, other_order, 0))
        kv_half = dw_kv.shape[0] // 2
        kv_block = second_exchange(*first_exchange(dw_kv[:kv_half], dw_kv[kv_half:]))
        d_x = d_hid.astype(F32) + dot(dq, wq_t, 1, 0) + dot(d_kv, wkv_t, 1, 0)
        d_x = d_x.astype(BF16).reshape(x_in.shape)

        dw_down = gather(dn_block) * grad_scale
        dw_up = gather(up_block) * grad_scale
        dw_o = gather(o_block) * grad_scale
        qkv = gather(jnp.concatenate([q_block, kv_block], axis=0))
        q_size = q_block.shape[0]
        qkv = qkv.reshape(dp_size * cp_size, q_size + kv_block.shape[0], width)
        dw_q = qkv[:, :q_size].reshape(-1, width) * grad_scale
        dw_kv = qkv[:, q_size:].reshape(-1, width) * grad_scale

        def weight_shape(grad_t, weight):
            return grad_t.reshape(weight.shape[1], weight.shape[2], width).transpose(2, 0, 1)

        kv_rows = kv_heads * head_dim
        return (d_x, weight_shape(dw_q, w_q), weight_shape(dw_kv[:kv_rows], w_k), weight_shape(dw_kv[kv_rows:], w_v), dw_o.reshape(w_o.shape), dw_up, dw_down)

    act_spec = P('dp', 'cp', None)
    return jax.shard_map(device_backward, mesh=mesh, in_specs=(act_spec, act_spec, P(), P(), P(), P(), P(), P()), out_specs=(act_spec, P(), P(), P(), P(), P(), P()), check_vma=False)
```
